32 devices in a mesh: dp: 1, sp: 32 (over x, y, z, core).
Axes of the slice: x: 2, y: 2, z: 4, core: 2. Of those that a mesh axis runs over, the one named last changes fastest.
Arguments:
- q: bfloat16 [32, 56, 128], P('dp')
- k: bfloat16 [32, 4096, 56, 128], P('dp', 'sp')
- v: bfloat16 [32, 4096, 56, 128], P('dp', 'sp')
Outputs:
- q: bfloat16 [32, 56, 128], P('dp')
All inputs are finite; a program needn't handle non-finite values.
Results may differ from the reference program's by a relative error of at most 0.012.
Values are sent between devices in bfloat16 or wider.
A program may use at most 2 GiB of HBM per device.

```python
import jax
import jax.numpy as jnp

BATCH = 32
CACHE = 4096
HEADS = 56
KV_HEADS = 56
HEAD = 128


def setup_inputs(seed: int = 0, part: int = 0) -> dict:
    kq, kk, kv = (jax.random.fold_in(k, part) for k in jax.random.split(jax.random.key(seed), 3))
    return {
        "q": (3 * jax.random.normal(kq, (BATCH, HEADS, HEAD), jnp.float32)).astype(jnp.bfloat16),
        "k": jax.random.normal(kk, (BATCH, CACHE, KV_HEADS, HEAD), jnp.float32).astype(jnp.bfloat16),
        "v": jax.random.normal(kv, (BATCH, CACHE, KV_HEADS, HEAD), jnp.float32).astype(jnp.bfloat16),
    }


def einsum(form, a, b):
    return jnp.einsum(form, a.astype(jnp.float32), b.astype(jnp.float32))


def reference(q, k, v):
    grouped = q.reshape(BATCH, KV_HEADS, -1, HEAD)
    scores = einsum("bgsd,bugd->bgsu", grouped, k) * HEAD**-0.5
    weights = jax.nn.softmax(scores, -1).astype(jnp.bfloat16)
    return einsum("bgsu,bugd->bgsd", weights, v).astype(jnp.bfloat16).reshape(BATCH, HEADS, HEAD)
```

```python
import functools

import jax
import jax.numpy as jnp
from jax import lax
from jax.experimental import pallas as pl
from jax.experimental.pallas import tpu as pltpu
from jax.sharding import PartitionSpec as P

N = 32
S = 32
H = 56
D = 128
G = 7
PAIRS = 64
SLOTS = 4
TAIL = 4
WHOLE = S - TAIL
UNITS = TAIL * G
LAG = 8
SCALE = D**-0.5 * 1.4426950408889634
F32 = jnp.float32
BF16 = jnp.bfloat16


def attend(q, kbuf, vbuf):
    qf = q.astype(F32)
    q2 = jnp.concatenate([qf, qf], 0).astype(BF16)
    col = lax.broadcasted_iota(jnp.int32, (16, 16 * PAIRS), 1)
    row = lax.broadcasted_iota(jnp.int32, (16, 16 * PAIRS), 0)
    mask = (col & 15) == row
    s, m = [], []
    for g in range(G):
        kg = kbuf[:, g].reshape(16 * PAIRS, D)
        x = lax.dot_general(q2[16 * g : 16 * g + 16], kg, (((1,), (1,)), ((), ())), preferred_element_type=F32)
        x = jnp.where(mask, x * SCALE, -jnp.inf)
        s.append(x)
        m.append(jnp.max(x, 1, keepdims=True))
    m = jnp.concatenate(m, 0)
    high = jnp.maximum(m[:H], m[H:])
    both = jnp.concatenate([high, high], 0)
    o, l = [], []
    for g in range(G):
        e = jnp.exp2(s[g] - both[16 * g : 16 * g + 16])
        l.append(jnp.sum(e, 1, keepdims=True))
        o.append(jnp.dot(e.astype(BF16), vbuf[:, g].reshape(16 * PAIRS, D), preferred_element_type=F32))
    l = jnp.concatenate(l, 0)
    o = jnp.concatenate(o, 0)
    return o[:H] + o[H:], high, l[:H] + l[H:]


def kernel(
    q_ref, k_hbm, v_hbm, out, kb, vb, snd, sst, own, uown, rsb, rst, rub, rut, wt,
    ksem, vsem, s_send, s_recv, st_send, st_recv, u_send, u_recv, ut_send, ut_recv, g_send, g_recv, h_send, h_recv,
):
    me = lax.axis_index("sp")

    def device(i):
        return {"sp": i}

    def fetch(s):
        slot = s % SLOTS
        return (
            pltpu.make_async_copy(k_hbm.at[s], kb.at[slot], ksem.at[slot]),
            pltpu.make_async_copy(v_hbm.at[s], vb.at[slot], vsem.at[slot]),
        )

    def start(s):
        for copy in fetch(s):
            copy.start()

    def taken(ref, sem):
        pltpu.make_async_copy(ref, ref, sem).wait()

    def send(src, dst, send_sem, recv_sem, to):
        pltpu.make_async_remote_copy(src, dst, send_sem, recv_sem, device_id=device(to), device_id_type=pl.DeviceIdType.MESH).start()

    for s in range(SLOTS - 1):
        start(s)
    barrier = pltpu.get_barrier_semaphore()

    @pl.loop(1, N)
    def _(i):
        pl.semaphore_signal(barrier, inc=1, device_id=device(lax.rem(me + i, N)), device_id_type=pl.DeviceIdType.MESH)

    def scales(stats):
        x = stats[...].reshape(N, D)
        high = jnp.max(x, 0, keepdims=True)
        e = jnp.exp2(x - high)
        lane = lax.broadcasted_iota(jnp.int32, (N, D), 1)
        e = jnp.where(lane < H, e, 0.0)
        total = jnp.sum(pltpu.roll(x, 64, 1) * e, 0, keepdims=True)
        lane = lax.broadcasted_iota(jnp.int32, (1, D), 1)
        total = jnp.where(lane < H, total, 1.0)
        wt[...] = (e / total).T

    def together(block, mine, w):
        acc = [None] * 4
        for i in range(N):
            x = jnp.where(me == i, mine, block(i).astype(F32)) * w[:, i : i + 1]
            acc[i % 4] = x if acc[i % 4] is None else acc[i % 4] + x
        return ((acc[0] + acc[1]) + (acc[2] + acc[3])).astype(BF16)

    def give_whole():
        taken(rst.at[pl.ds(0, N - 1)], st_recv)
        taken(rsb.at[pl.ds(0, N - 1)], s_recv)
        scales(rst)
        for g in range(G):
            out[me, g] = together(lambda i: rsb[i, g], own[g], wt[8 * g : 8 * g + 8])

        @pl.loop(1, N)
        def _(i):
            send(out.at[me], out.at[me], g_send, g_recv.at[me], lax.rem(me + i, N))

    def give_unit():
        u = lax.rem(me + TAIL, N)
        s, g = WHOLE + u // G, u % G
        taken(rut.at[pl.ds(0, N - 1)], ut_recv)
        taken(rub.at[pl.ds(0, N - 1)], u_recv)
        scales(rut)
        out[s, g] = together(lambda i: rub[i], uown[...], wt[pl.ds(pl.multiple_of(8 * g, 8), 8)])

        @pl.loop(1, N)
        def _(i):
            send(out.at[s, g], out.at[s, g], h_send, h_recv, lax.rem(me + i, N))

    def work(s):
        slot = s % SLOTS
        for copy in fetch(s):
            copy.wait()
        o, m, l = attend(q_ref[s], kb.at[slot], vb.at[slot])
        row = lax.broadcasted_iota(jnp.int32, (H, D), 0)
        lane = lax.broadcasted_iota(jnp.int32, (H, D), 1)
        stats = jnp.sum(jnp.where(lane == row, m, jnp.where(lane == row + 64, l, 0.0)), 0, keepdims=True)
        sst[s] = stats
        o = o.reshape(G, 8, D)
        snd[s] = o.astype(BF16)
        return o, stats

    @pl.loop(0, WHOLE)
    def _(s):
        @pl.when(s + SLOTS - 1 < S)
        def _():
            start(s + SLOTS - 1)

        o, stats = work(s)

        @pl.when(s == 0)
        def _():
            pl.semaphore_wait(barrier, N - 1)

        @pl.when(s == me)
        def _():
            own[...] = o
            rst[me] = stats
            rsb[me] = snd[s]

        @pl.when(s != me)
        def _():
            send(sst.at[s], rst.at[me], st_send, st_recv, s)
            send(snd.at[s], rsb.at[me], s_send, s_recv, s)

        @pl.when(s == me + LAG)
        def _():
            give_whole()

    @pl.loop(WHOLE, S)
    def _(s):
        @pl.when(s + SLOTS - 1 < S)
        def _():
            start(s + SLOTS - 1)

        o, stats = work(s)
        for g in range(G):
            to = lax.rem((s - WHOLE) * G + g + N - TAIL, N)

            @pl.when(to == me)
            def _():
                uown[...] = o[g]
                rut[me] = stats
                rub[me] = snd[s, g]

            @pl.when(to != me)
            def _():
                send(sst.at[s], rut.at[me], ut_send, ut_recv, to)
                send(snd.at[s, g], rub.at[me], u_send, u_recv, to)

        @pl.when((s == me + LAG) & (me < WHOLE))
        def _():
            give_whole()

    @pl.when((me >= S - LAG) & (me < WHOLE))
    def _():
        give_whole()

    units = (me < WHOLE - TAIL) | (me >= WHOLE)

    @pl.when(units)
    def _():
        give_unit()

    @pl.loop(0, WHOLE)
    def _(s):
        @pl.when(s != me)
        def _():
            taken(out.at[s], g_recv.at[s])

    @pl.when(me < WHOLE)
    def _():
        taken(snd.at[pl.ds(0, WHOLE - 1)], s_send)
        taken(sst.at[pl.ds(0, WHOLE - 1)], st_send)
        taken(out.at[pl.ds(0, N - 1)], g_send)

    @pl.when(me >= WHOLE)
    def _():
        taken(snd.at[pl.ds(0, WHOLE)], s_send)
        taken(sst.at[pl.ds(0, WHOLE)], st_send)

    @pl.when(units)
    def _():
        taken(rub.at[pl.ds(0, UNITS - 1)], u_send)
        taken(rut.at[pl.ds(0, UNITS - 1)], ut_send)
        taken(rub.at[pl.ds(0, N - 1)], h_send)
        taken(rub.at[pl.ds(0, UNITS - 1)], h_recv)

    @pl.when(jnp.logical_not(units))
    def _():
        taken(rub.at[pl.ds(0, UNITS)], u_send)
        taken(rut.at[pl.ds(0, UNITS)], ut_send)
        taken(rub.at[pl.ds(0, UNITS)], h_recv)


def solution(mesh):
    def step(q, k, v):
        dma = pltpu.SemaphoreType.DMA
        vmem = pltpu.VMEM
        out = pl.pallas_call(
            kernel,
            out_shape=jax.ShapeDtypeStruct((S, G, 8, D), BF16),
            in_specs=[
                pl.BlockSpec(memory_space=pltpu.VMEM),
                pl.BlockSpec(memory_space=pl.ANY),
                pl.BlockSpec(memory_space=pl.ANY),
            ],
            out_specs=pl.BlockSpec(memory_space=pltpu.VMEM),
            scratch_shapes=[
                vmem((SLOTS, PAIRS, G, 16, D), BF16),
                vmem((SLOTS, PAIRS, G, 16, D), BF16),
                vmem((S, G, 8, D), BF16),
                vmem((S, 1, D), F32),
                vmem((G, 8, D), F32),
                vmem((8, D), F32),
                vmem((N, G, 8, D), BF16),
                vmem((N, 1, D), F32),
                vmem((N, 8, D), BF16),
                vmem((N, 1, D), F32),
                vmem((D, N), F32),
                dma((SLOTS,)),
                dma((SLOTS,)),
            ]
            + [dma(())] * 9 + [dma((WHOLE,))] + [dma(())] * 2,
            compiler_params=pltpu.CompilerParams(collective_id=0, has_side_effects=True, vmem_limit_bytes=60 * 2**20),
            cost_estimate=pl.CostEstimate(flops=4 * S * 128 * H * D, bytes_accessed=2 * 2 * S * 128 * H * D, transcendentals=0),
        )(q, k.reshape(S, PAIRS, G, 16, D), v.reshape(S, PAIRS, G, 16, D))
        return out.reshape(q.shape)

    return jax.shard_map(
        step,
        mesh=mesh,
        in_specs=(P("dp", None, None), P("dp", "sp", None, None), P("dp", "sp", None, None)),
        out_specs=P("dp", None, None),
        check_vma=False,
    )
```

```python
import functools

import jax
import jax.numpy as jnp
from jax import lax
from jax.experimental import pallas as pl
from jax.experimental.pallas import tpu as pltpu
from jax.sharding import PartitionSpec as P

N = 32
S = 32
H = 56
D = 128
G = 7
PAIRS = 64
SLOTS = 8
FINE = 12
WHOLE = S - FINE
SIZES = (32, 32, 16, 4)
FIRST = (0, 32, 64, 80)
ROUNDS = len(SIZES)
LAG = 9
GREET = 3
SPREAD, BACK = 5, 13
SCALE = D**-0.5 * 1.4426950408889634
F32 = jnp.float32
BF16 = jnp.bfloat16


def attend(q, kbuf, vbuf):
    qf = q.astype(F32)
    q2 = jnp.concatenate([qf, qf], 0).astype(BF16)
    col = lax.broadcasted_iota(jnp.int32, (16, 16 * PAIRS), 1)
    row = lax.broadcasted_iota(jnp.int32, (16, 16 * PAIRS), 0)
    mask = (col & 15) == row
    s, m = [], []
    for g in range(G):
        kg = kbuf[:, g].reshape(16 * PAIRS, D)
        x = lax.dot_general(q2[16 * g : 16 * g + 16], kg, (((1,), (1,)), ((), ())), preferred_element_type=F32)
        x = jnp.where(mask, x * SCALE, -jnp.inf)
        s.append(x)
        m.append(jnp.max(x, 1, keepdims=True))
    m = jnp.concatenate(m, 0)
    high = jnp.maximum(m[:H], m[H:])
    both = jnp.concatenate([high, high], 0)
    o, l = [], []
    for g in range(G):
        e = jnp.exp2(s[g] - both[16 * g : 16 * g + 16])
        l.append(jnp.sum(e, 1, keepdims=True))
        o.append(jnp.dot(e.astype(BF16), vbuf[:, g].reshape(16 * PAIRS, D), preferred_element_type=F32))
    l = jnp.concatenate(l, 0)
    o = jnp.concatenate(o, 0)
    return o[:H] + o[H:], high, l[:H] + l[H:]


def kernel(
    q_hbm, k_hbm, v_hbm, out, q_ref, q_sem, kb, vb, snd, sst, own, uown, rsb, rst, rub, rut, wt,
    ksem, vsem, s_send, s_recv, st_send, st_recv, u_send, u_recv, ut_send, ut_recv, g_send, g_recv, h_send, h_recv,
):
    me = lax.axis_index("sp")
    mine = lax.rem(BACK * me, N)
    turn = lax.rem(mine + N - WHOLE, N)
    middle = lax.rem(me, 8)
    centre = jnp.where((middle >= 2) & (middle < 6), me // 8 * 4 + middle - 2, N)

    def owner(s):
        return lax.rem(SPREAD * s, N)

    def place(c):
        return turn if c < 2 else centre

    def locate(n):
        outer = lax.rem(SPREAD * (n + WHOLE), N)
        inner = lax.rem(n, 16) // 4 * 8 + 2 + lax.rem(n, 4)
        return n // FIRST[1] + n // FIRST[3], outer + n // FIRST[2] * (inner - outer)

    def device(i):
        return {"sp": i}

    def fetch(s):
        slot = s % SLOTS
        return (
            pltpu.make_async_copy(k_hbm.at[s], kb.at[slot], ksem.at[slot]),
            pltpu.make_async_copy(v_hbm.at[s], vb.at[slot], vsem.at[slot]),
        )

    def start(s):
        for copy in fetch(s):
            copy.start()

    def taken(ref, sem):
        pltpu.make_async_copy(ref, ref, sem).wait()

    def send(src, dst, send_sem, recv_sem, to):
        pltpu.make_async_remote_copy(src, dst, send_sem, recv_sem, device_id=device(to), device_id_type=pl.DeviceIdType.MESH).start()

    start(0)
    q_copy = pltpu.make_async_copy(q_hbm, q_ref, q_sem)
    q_copy.start()
    for s in range(1, SLOTS - 1):
        start(s)
    barrier = pltpu.get_barrier_semaphore()

    @pl.loop(1, N)
    def _(i):
        pl.semaphore_signal(barrier, inc=1, device_id=device(lax.rem(me + i, N)), device_id_type=pl.DeviceIdType.MESH)

    q_copy.wait()

    def scales(stats):
        x = stats[...].reshape(N, D)
        high = jnp.max(x, 0, keepdims=True)
        e = jnp.exp2(x - high)
        lane = lax.broadcasted_iota(jnp.int32, (N, D), 1)
        e = jnp.where(lane < H, e, 0.0)
        total = jnp.sum(pltpu.roll(x, 64, 1) * e, 0, keepdims=True)
        lane = lax.broadcasted_iota(jnp.int32, (1, D), 1)
        total = jnp.where(lane < H, total, 1.0)
        wt[...] = (e / total).T

    def together(block, own_part, w):
        acc = [None] * 4
        for i in range(N):
            x = jnp.where(me == i, own_part, block(i).astype(F32)) * w[:, i : i + 1]
            acc[i % 4] = x if acc[i % 4] is None else acc[i % 4] + x
        return ((acc[0] + acc[1]) + (acc[2] + acc[3])).astype(BF16)

    def give_whole():
        taken(rst.at[pl.ds(0, N - 1)], st_recv)
        taken(rsb.at[pl.ds(0, N - 1)], s_recv)
        scales(rst)
        for g in range(G):
            out[mine, g] = together(lambda i: rsb[i, g], own[g], wt[8 * g : 8 * g + 8])

        @pl.loop(1, N)
        def _(i):
            send(out.at[mine], out.at[mine], g_send, g_recv.at[mine], lax.rem(me + i, N))

    def give_unit(c):
        u = FIRST[c] + place(c)
        s, g = WHOLE + u // G, lax.rem(u, G)
        taken(rut.at[c, pl.ds(0, N - 1)], ut_recv.at[c])
        taken(rub.at[c, pl.ds(0, N - 1)], u_recv.at[c])
        scales(rut.at[c])
        out[s, g] = together(lambda i: rub[c, i], uown[c], wt[pl.ds(pl.multiple_of(8 * g, 8), 8)])

        for i in range(1, N):
            send(out.at[s, g], out.at[s, g], h_send.at[c], h_recv.at[c], lax.rem(me + i, N))

    def send_whole(s):
        @pl.when(s != mine)
        def _():
            to = owner(s)
            send(sst.at[s], rst.at[me], st_send, st_recv, to)
            send(snd.at[s], rsb.at[me], s_send, s_recv, to)

    def work(s):
        slot = s % SLOTS
        for copy in fetch(s):
            copy.wait()
        o, m, l = attend(q_ref[s], kb.at[slot], vb.at[slot])
        row = lax.broadcasted_iota(jnp.int32, (H, D), 0)
        lane = lax.broadcasted_iota(jnp.int32, (H, D), 1)
        stats = jnp.sum(jnp.where(lane == row, m, jnp.where(lane == row + 64, l, 0.0)), 0, keepdims=True)
        sst[s] = stats
        o = o.reshape(G, 8, D)
        snd[s] = o.astype(BF16)
        return o, stats

    @pl.loop(0, WHOLE)
    def _(s):
        @pl.when(s + SLOTS - 1 < S)
        def _():
            start(s + SLOTS - 1)

        o, stats = work(s)

        @pl.when(s == mine)
        def _():
            own[...] = o
            rst[me] = stats
            rsb[me] = snd[s]

        @pl.when(s == GREET)
        def _():
            pl.semaphore_wait(barrier, N - 1)
            for t in range(GREET):
                send_whole(t)

        @pl.when(s >= GREET)
        def _():
            send_whole(s)

        @pl.when(s == mine + LAG)
        def _():
            give_whole()

    @pl.loop(WHOLE, S)
    def _(s):
        @pl.when(s + SLOTS - 1 < S)
        def _():
            start(s + SLOTS - 1)

        o, stats = work(s)
        for g in range(G):
            n = (s - WHOLE) * G + g
            c, to = locate(n)

            @pl.when(to == me)
            def _():
                uown[c] = o[g]
                rut[c, me] = stats
                rub[c, me] = snd[s, g]

            @pl.when(to != me)
            def _():
                send(sst.at[s], rut.at[c, me], ut_send.at[c], ut_recv.at[c], to)
                send(snd.at[s, g], rub.at[c, me], u_send.at[c], u_recv.at[c], to)

        @pl.when((s == mine + LAG) & (mine < WHOLE))
        def _():
            give_whole()

    @pl.when((mine >= S - LAG) & (mine < WHOLE))
    def _():
        give_whole()

    for c in range(ROUNDS):

        @pl.when(place(c) < SIZES[c])
        def _(c=c):
            give_unit(c)

    @pl.loop(0, WHOLE)
    def _(s):
        @pl.when(s != mine)
        def _():
            taken(out.at[s], g_recv.at[s])

    @pl.when(mine < WHOLE)
    def _():
        taken(snd.at[pl.ds(0, WHOLE - 1)], s_send)
        taken(sst.at[pl.ds(0, WHOLE - 1)], st_send)
        taken(out.at[pl.ds(0, N - 1)], g_send)

    @pl.when(mine >= WHOLE)
    def _():
        taken(snd.at[pl.ds(0, WHOLE)], s_send)
        taken(sst.at[pl.ds(0, WHOLE)], st_send)

    for c in range(ROUNDS):

        def settle(c, sent):
            taken(rub.at[c, pl.ds(0, sent)], u_send.at[c])
            taken(rut.at[c, pl.ds(0, sent)], ut_send.at[c])
            taken(rub.at[c, pl.ds(0, sent)], h_recv.at[c])

        @pl.when(place(c) < SIZES[c])
        def _(c=c):
            settle(c, SIZES[c] - 1)
            taken(rub.at[c, pl.ds(0, N - 1)], h_send.at[c])

        if SIZES[c] < N:

            @pl.when(place(c) >= SIZES[c])
            def _(c=c):
                settle(c, SIZES[c])


def solution(mesh):
    def step(q, k, v):
        dma = pltpu.SemaphoreType.DMA
        vmem = pltpu.VMEM
        out = pl.pallas_call(
            kernel,
            out_shape=jax.ShapeDtypeStruct((S, G, 8, D), BF16),
            in_specs=[
                pl.BlockSpec(memory_space=pltpu.HBM),
                pl.BlockSpec(memory_space=pl.ANY),
                pl.BlockSpec(memory_space=pl.ANY),
            ],
            out_specs=pl.BlockSpec(memory_space=pltpu.VMEM),
            scratch_shapes=[
                vmem((S, H, D), BF16),
                dma(()),
                vmem((SLOTS, PAIRS, G, 16, D), BF16),
                vmem((SLOTS, PAIRS, G, 16, D), BF16),
                vmem((S, G, 8, D), BF16),
                vmem((S, 1, D), F32),
                vmem((G, 8, D), F32),
                vmem((ROUNDS, 8, D), F32),
                vmem((N, G, 8, D), BF16),
                vmem((N, 1, D), F32),
                vmem((ROUNDS, N, 8, D), BF16),
                vmem((ROUNDS, N, 1, D), F32),
                vmem((D, N), F32),
                dma((SLOTS,)),
                dma((SLOTS,)),
            ]
            + [dma(())] * 4 + [dma((ROUNDS,))] * 4 + [dma(()), dma((WHOLE,))] + [dma((ROUNDS,))] * 2,
            compiler_params=pltpu.CompilerParams(collective_id=0, has_side_effects=True, vmem_limit_bytes=40 * 2**20),
            cost_estimate=pl.CostEstimate(flops=4 * S * 128 * H * D, bytes_accessed=2 * 2 * S * 128 * H * D, transcendentals=0),
        )(q, k.reshape(S, PAIRS, G, 16, D), v.reshape(S, PAIRS, G, 16, D))
        return out.reshape(q.shape)

    return jax.shard_map(
        step,
        mesh=mesh,
        in_specs=(P("dp", None, None), P("dp", "sp", None, None), P("dp", "sp", None, None)),
        out_specs=P("dp", None, None),
        check_vma=False,
    )
```

```python
import functools

import jax
import jax.numpy as jnp
from jax import lax
from jax.experimental import pallas as pl
from jax.experimental.pallas import tpu as pltpu
from jax.sharding import PartitionSpec as P

N = 32
S = 32
H = 56
D = 128
G = 7
PAIRS = 64
SLOTS = 8
GRANT = 55888896
FINE = 12
WHOLE = S - FINE
COUNTS = (4, 4, 2, 2)
BEGINS = (20, 24, 28, 30)
ROUNDS = len(COUNTS)
SIZES = tuple(G * n for n in COUNTS)
LAG = 8
GREET = 3
SPREAD, BACK = 5, 13
SCALE = D**-0.5 * 1.4426950408889634
F32 = jnp.float32
BF16 = jnp.bfloat16


def attend(q, kbuf, vbuf):
    qf = q.astype(F32).reshape(H, D)
    q2 = jnp.concatenate([qf, qf], 0).astype(BF16)
    col = lax.broadcasted_iota(jnp.int32, (16, 16 * PAIRS), 1)
    row = lax.broadcasted_iota(jnp.int32, (16, 16 * PAIRS), 0)
    mask = (col & 15) == row
    x = [
        lax.dot_general(q2[16 * g : 16 * g + 16], kbuf[:, g].reshape(16 * PAIRS, D), (((1,), (1,)), ((), ())), preferred_element_type=F32)
        for g in range(G)
    ]
    e, m, l = [], [], []
    for g in range(G):
        y = jnp.where(mask, x[g] * SCALE, -jnp.inf)
        m.append(jnp.max(y, 1, keepdims=True))
        y = jnp.exp2(y - m[g])
        l.append(jnp.sum(y, 1, keepdims=True))
        e.append(y.astype(BF16))
    o = [jnp.dot(e[g], vbuf[:, g].reshape(16 * PAIRS, D), preferred_element_type=F32) for g in range(G)]
    o, m, l = (jnp.concatenate(part, 0) for part in (o, m, l))
    high = jnp.maximum(m[:H], m[H:])
    even, odd = jnp.exp2(m[:H] - high), jnp.exp2(m[H:] - high)
    return o[:H] * even + o[H:] * odd, high, l[:H] * even + l[H:] * odd


def kernel(
    q_hbm, k_hbm, v_hbm, out, q_ref, q_sem, kb, vb, snd, sst, own, uown, rsb, rst, rub, rut, wt,
    ksem, vsem, s_send, s_recv, st_send, st_recv, u_send, u_recv, ut_send, ut_recv, g_send, g_recv, h_send, h_recv,
):
    me = lax.axis_index("sp")
    mine = lax.rem(BACK * me, N)
    turn = lax.rem(mine + N - WHOLE, N)
    middle = lax.rem(me, 8)
    centre = jnp.where((middle >= 2) & (middle < 6), me // 8 * 4 + middle - 2, N)

    def owner(s):
        return lax.rem(SPREAD * s, N)

    def place(c):
        return turn if c < 2 else centre

    def unit_owner(c, u):
        if c < 2:
            return lax.rem(SPREAD * u + SPREAD * WHOLE, N)
        return u + 2 + u // 4 * 4

    def device(i):
        return {"sp": i}

    def fetch(s):
        slot = s % SLOTS
        return (
            pltpu.make_async_copy(k_hbm.at[s], kb.at[slot], ksem.at[slot]),
            pltpu.make_async_copy(v_hbm.at[s], vb.at[slot], vsem.at[slot]),
        )

    def start(s):
        for copy in fetch(s):
            copy.start()

    def taken(ref, sem):
        pltpu.make_async_copy(ref, ref, sem).wait()

    def send(src, dst, send_sem, recv_sem, to):
        pltpu.make_async_remote_copy(src, dst, send_sem, recv_sem, device_id=device(to), device_id_type=pl.DeviceIdType.MESH).start()

    q_copy = pltpu.make_async_copy(q_hbm, q_ref, q_sem)
    q_copy.start()
    start(0)
    barrier = pltpu.get_barrier_semaphore()

    @pl.loop(1, N)
    def _(i):
        pl.semaphore_signal(barrier, inc=1, device_id=device(lax.rem(me + i, N)), device_id_type=pl.DeviceIdType.MESH)

    q_copy.wait()
    for s in range(1, SLOTS - 1):
        start(s)

    def scales(stats):
        x = stats[...].reshape(N, D)
        high = jnp.max(x, 0, keepdims=True)
        e = jnp.exp2(x - high)
        lane = lax.broadcasted_iota(jnp.int32, (N, D), 1)
        e = jnp.where(lane < H, e, 0.0)
        total = jnp.sum(pltpu.roll(x, 64, 1) * e, 0, keepdims=True)
        lane = lax.broadcasted_iota(jnp.int32, (1, D), 1)
        total = jnp.where(lane < H, total, 1.0)
        wt[...] = (e / total).T

    def together(block, own_part, w):
        acc = [None] * 4
        for i in range(N):
            x = jnp.where(me == i, own_part, block(i).astype(F32)) * w[:, i : i + 1]
            acc[i % 4] = x if acc[i % 4] is None else acc[i % 4] + x
        return ((acc[0] + acc[1]) + (acc[2] + acc[3])).astype(BF16)

    def give_whole():
        taken(rst.at[pl.ds(0, N - 1)], st_recv)
        taken(rsb.at[pl.ds(0, N - 1)], s_recv)
        scales(rst)
        for g in range(G):
            out[mine, g] = together(lambda i: rsb[i, g], own[g], wt[8 * g : 8 * g + 8])

        @pl.loop(1, N)
        def _(i):
            send(out.at[mine], out.at[mine], g_send, g_recv.at[mine], lax.rem(me + i, N))

    def give_unit(c):
        s, g = BEGINS[c] + place(c) // G, lax.rem(place(c), G)
        taken(rut.at[c, pl.ds(0, N - 1)], ut_recv.at[c])
        taken(rub.at[c, pl.ds(0, N - 1)], u_recv.at[c])
        scales(rut.at[c])
        out[s, g] = together(lambda i: rub[c, i], uown[c], wt[pl.ds(pl.multiple_of(8 * g, 8), 8)])

        for i in range(1, N):
            send(out.at[s, g], out.at[s, g], h_send.at[c], h_recv.at[c], lax.rem(me + i, N))

    def send_whole(s):
        @pl.when(s != mine)
        def _():
            to = owner(s)
            send(sst.at[s], rst.at[me], st_send, st_recv, to)
            send(snd.at[s], rsb.at[me], s_send, s_recv, to)

    def work(s):
        slot = s % SLOTS
        for copy in fetch(s):
            copy.wait()
        o, m, l = attend(q_ref[s], kb.at[slot], vb.at[slot])
        row = lax.broadcasted_iota(jnp.int32, (H, D), 0)
        lane = lax.broadcasted_iota(jnp.int32, (H, D), 1)
        stats = jnp.sum(jnp.where(lane == row, m, jnp.where(lane == row + 64, l, 0.0)), 0, keepdims=True)
        sst[s] = stats
        o = o.reshape(G, 8, D)
        snd[s] = o.astype(BF16)
        return o, stats

    @pl.loop(0, WHOLE)
    def _(s):
        @pl.when(s + SLOTS - 1 < S)
        def _():
            start(s + SLOTS - 1)

        o, stats = work(s)

        @pl.when(s == mine)
        def _():
            own[...] = o
            rst[me] = stats
            rsb[me] = snd[s]

        @pl.when(s == GREET)
        def _():
            pl.semaphore_wait(barrier, N - 1)
            for t in range(GREET):
                send_whole(t)

        @pl.when(s >= GREET)
        def _():
            send_whole(s)

        @pl.when(s == mine + LAG)
        def _():
            give_whole()

    for c in range(ROUNDS):

        @pl.loop(BEGINS[c], BEGINS[c] + COUNTS[c])
        def _(s, c=c):
            @pl.when(s + SLOTS - 1 < S)
            def _():
                start(s + SLOTS - 1)

            o, stats = work(s)
            for g in range(G):
                to = unit_owner(c, (s - BEGINS[c]) * G + g)

                @pl.when(to == me)
                def _(g=g):
                    uown[c] = o[g]
                    rut[c, me] = stats
                    rub[c, me] = snd[s, g]

                @pl.when(to != me)
                def _(g=g, to=to):
                    send(snd.at[s, g], rub.at[c, me], u_send.at[c], u_recv.at[c], to)
                    send(sst.at[s], rut.at[c, me], ut_send.at[c], ut_recv.at[c], to)

            if BEGINS[c] < WHOLE + LAG:

                @pl.when((s == mine + LAG) & (mine < WHOLE))
                def _():
                    give_whole()

    for c in range(ROUNDS):

        @pl.when(place(c) < SIZES[c])
        def _(c=c):
            give_unit(c)

    @pl.loop(0, WHOLE)
    def _(s):
        @pl.when(s != mine)
        def _():
            taken(out.at[s], g_recv.at[s])

    @pl.when(mine < WHOLE)
    def _():
        taken(snd.at[pl.ds(0, WHOLE - 1)], s_send)
        taken(sst.at[pl.ds(0, WHOLE - 1)], st_send)
        taken(out.at[pl.ds(0, N - 1)], g_send)

    @pl.when(mine >= WHOLE)
    def _():
        taken(snd.at[pl.ds(0, WHOLE)], s_send)
        taken(sst.at[pl.ds(0, WHOLE)], st_send)

    for c in range(ROUNDS):

        def settle(c, sent):
            taken(rub.at[c, pl.ds(0, sent)], u_send.at[c])
            taken(rut.at[c, pl.ds(0, sent)], ut_send.at[c])
            taken(rub.at[c, pl.ds(0, sent)], h_recv.at[c])

        @pl.when(place(c) < SIZES[c])
        def _(c=c):
            settle(c, SIZES[c] - 1)
            taken(rub.at[c, pl.ds(0, N - 1)], h_send.at[c])

        if SIZES[c] < N:

            @pl.when(place(c) >= SIZES[c])
            def _(c=c):
                settle(c, SIZES[c])


def solution(mesh):
    def step(q, k, v):
        dma = pltpu.SemaphoreType.DMA
        vmem = pltpu.VMEM
        out = pl.pallas_call(
            kernel,
            out_shape=jax.ShapeDtypeStruct((S, G, 8, D), BF16),
            in_specs=[
                pl.BlockSpec(memory_space=pl.ANY),
                pl.BlockSpec(memory_space=pl.ANY),
                pl.BlockSpec(memory_space=pl.ANY),
            ],
            out_specs=pl.BlockSpec(memory_space=pltpu.VMEM),
            scratch_shapes=[
                vmem((S, G, 8, D), BF16),
                dma(()),
                vmem((SLOTS, PAIRS, G, 16, D), BF16),
                vmem((SLOTS, PAIRS, G, 16, D), BF16),
                vmem((S, G, 8, D), BF16),
                vmem((S, 1, D), F32),
                vmem((G, 8, D), F32),
                vmem((ROUNDS, 8, D), F32),
                vmem((N, G, 8, D), BF16),
                vmem((N, 1, D), F32),
                vmem((ROUNDS, N, 8, D), BF16),
                vmem((ROUNDS, N, 1, D), F32),
                vmem((D, N), F32),
                dma((SLOTS,)),
                dma((SLOTS,)),
            ]
            + [dma(())] * 4 + [dma((ROUNDS,))] * 4 + [dma(()), dma((WHOLE,))] + [dma((ROUNDS,))] * 2,
            compiler_params=pltpu.CompilerParams(collective_id=0, has_side_effects=True, vmem_limit_bytes=GRANT),
            cost_estimate=pl.CostEstimate(flops=4 * S * 128 * H * D, bytes_accessed=2 * 2 * S * 128 * H * D, transcendentals=0),
        )(q.reshape(S, G, 8, D), k.reshape(S, PAIRS, G, 16, D), v.reshape(S, PAIRS, G, 16, D))
        return out.reshape(q.shape)

    return jax.shard_map(
        step,
        mesh=mesh,
        in_specs=(P("dp", None, None), P("dp", "sp", None, None), P("dp", "sp", None, None)),
        out_specs=P("dp", None, None),
        check_vma=False,
    )
```
